32 devices in a mesh: dp: 4 (over x, core), expert: 8 (over z, y).
Axes of the slice: x: 2, y: 2, z: 4, core: 2. Of those that a mesh axis runs over, the one named last changes fastest.
Arguments:
- tokens: bfloat16 [4096, 1024], P(('dp', 'expert')), may hold values from -6 to 6
- task_ids: int32 [32], P('dp'), may hold values from 0 to 5
- routing: int32 [32, 2], P('dp'), may hold values from 0 to 7, all different within a row; in each aligned block of 8 rows (0 to 7, 8 to 15, ...) at most 3 rows name the same one
- gate_weight: bfloat16 [1024, 48], replicated, may hold values from -0.1875 to 0.1875
- w_in: bfloat16 [8, 1024, 4096], P('expert', None, 'dp'), may hold values from -0.1875 to 0.1875
- w_out: bfloat16 [8, 4096, 1024], P('expert', 'dp'), may hold values from -0.09375 to 0.09375
Outputs:
- mixed: bfloat16 [4096, 1024], P(('dp', 'expert'))
The draws below stay inside these ranges and needn't reach their ends.
Inputs may be any that keep to these rules, and one draw needn't show every extreme that they name: `routing`: each row names two different experts. Within the 8 blocks of one index of dp no expert is named more than 3 times, a bound that some block reaches.
All inputs are finite; a program needn't handle non-finite values.
Results may differ from the reference program's by a relative error of at most 0.015.
Values may be sent and summed in bfloat16 or wider, within the bound.
A program may use at most 64 MiB of HBM per device.

```python
import math
import jax
import jax.numpy as jnp
import numpy as np
from jax import lax

D = 1024
FF = 4096
TASKS = 6
BLK = 128
EXPERTS = 8
ROWBLK = 8
CAP = 3
BLOCKS = 32
TOKENS = 4096
N_DP = 4


def with_ends(array, stream_key, smallest, high):
    extent = array.shape
    index_at = [jax.random.randint(jax.random.fold_in(stream_key, axis), (), 0, extent[axis]) for axis in range(len(extent))]
    array = array.at[tuple(index_at)].set(smallest)
    longest = extent.index(max(extent))
    index_at[longest] = (index_at[longest] + 1) % extent[longest]
    return array.at[tuple(index_at)].set(high)


def level_of(stream_key, shape, shards, smallest, largest):
    def one(dim, blocks):
        draws = jax.random.uniform(jax.random.fold_in(jax.random.fold_in(stream_key, 6), dim), (blocks,), jnp.float32, smallest / len(shards), largest / len(shards))
        return jnp.repeat(jnp.exp(draws), shape[dim] // blocks).reshape((-1,) + (1,) * (len(shape) - dim - 1))

    loudness = one(*shards[0])
    for cut in shards[1:]:
        loudness = loudness * one(*cut)
    return loudness


def routed_block(key, own, number, rows, count, top, most, lean):
    sequence = jax.random.permutation(key, count)
    heavy_load, ordinary = load_shares(count, rows * top, most, lean, True), load_shares(count, rows * top, most, lean, False)
    places = jnp.arange(count)

    def named(tallies, offset_by):
        used = int((tallies > 0).sum())
        fixed = max(1, used // 4)
        shifted = fixed + (places - fixed + offset_by * (used - fixed)) % max(1, count - fixed)
        return jnp.zeros((count,), jnp.int32).at[sequence[jnp.where(places < fixed, places, shifted)]].set(jnp.asarray(tallies, jnp.int32))

    tallies = jnp.where(number % 4 == 0, named(heavy_load, number // 4), named(ordinary, number - number // 4 - 1))
    mixed = jax.random.permutation(jax.random.fold_in(own, 3), count)
    source_of, taker = mixed[0:count // 2 * 2:2], mixed[1:count // 2 * 2:2]
    slack = jnp.minimum(tallies[source_of] - 1, most - tallies[taker]) // 2
    slack = jnp.where((source_of == sequence[0]) | (taker == sequence[0]) | (tallies[taker] == 0), 0, jnp.maximum(slack, 0))
    shifted = jax.random.randint(jax.random.fold_in(own, 4), (count // 2,), 0, 1 << 20) % (slack + 1)
    tallies = tallies.at[source_of].add(-shifted).at[taker].add(shifted)
    members = jnp.searchsorted(jnp.cumsum(tallies), jnp.arange(rows * top), side="right").astype(jnp.int32)
    table = members.reshape(top, rows).T
    table = table[jax.random.permutation(jax.random.fold_in(own, 1), rows)]
    offset_by = jax.random.randint(jax.random.fold_in(own, 2), (rows, 1), 0, top)
    return jnp.take_along_axis(table, (jnp.arange(top)[None, :] + offset_by) % top, axis=1)


def load_shares(count, total, bound, slope, full):
    weights = [(1 << 20) // math.isqrt(grade ** slope) + 1 for grade in range(1, count + 1)]
    largest = bound if full else min(bound, max(-(-total // count), total * weights[0] // sum(weights)))
    least = 1 if total - largest >= count - 1 else 0
    given, surplus = [largest] + [least] * (count - 1), total - largest - least * (count - 1)
    while surplus > 0:
        candidates = [i for i in range(1, count) if given[i] < largest] or [i for i in range(1, count) if given[i] < bound]
        mass, left = sum([weights[i] for i in candidates]), surplus
        for i in candidates:
            addition = min(bound - given[i], max(1, left * weights[i] // mass), surplus)
            given[i] = given[i] + addition
            surplus = surplus - addition
    return np.array(given)


def bell_draw(stream_key, dims, width, most, shards=(), dtype=jnp.bfloat16):
    level = level_of(stream_key, dims, shards, -0.22, 0.18) if shards else 1.0
    entries = jax.random.normal(stream_key, dims, jnp.float32) * width * level
    return jnp.minimum(jnp.maximum(entries, -most), most).astype(dtype)


def setup_inputs(seed: int = 0) -> dict:
    splits = jax.random.split(jax.random.key(seed), 7)
    tokens = bell_draw(splits[0], (TOKENS, D), 1.0, 6.0, ((0, 32),))
    task_ids = with_ends(jax.random.randint(splits[1], (BLOCKS,), 0, TASKS), jax.random.fold_in(splits[1], 1), 0, TASKS - 1).astype(jnp.int32)
    routing_keys = jax.random.split(jax.random.fold_in(splits[2], 1), BLOCKS // ROWBLK)
    routing_turns = jax.random.permutation(jax.random.fold_in(splits[2], 3), BLOCKS // ROWBLK)
    routing = jax.vmap(lambda own, number: routed_block(jax.random.fold_in(splits[2], 2), own, number, ROWBLK, EXPERTS, 2, CAP, 2))(routing_keys, routing_turns).reshape((BLOCKS, 2))
    gate_weight = bell_draw(splits[3], (D, TASKS * EXPERTS), D ** -0.5, 0.1875)
    w_in = bell_draw(splits[4], (EXPERTS, D, FF), D ** -0.5, 0.1875, ((0, 8), (2, 4)))
    w_out = bell_draw(splits[5], (EXPERTS, FF, D), FF ** -0.5, 0.09375, ((0, 8), (1, 4)))
    return dict(tokens=tokens, task_ids=task_ids, routing=routing, gate_weight=gate_weight, w_in=w_in, w_out=w_out)


def expert_output(block_rows, expert_id, w_in, w_out):
    hidden = jax.nn.gelu(jnp.dot(block_rows, w_in[expert_id], preferred_element_type=jnp.float32)).astype(jnp.bfloat16)
    slice_width = FF // N_DP
    hidden_split = hidden.reshape(BLK, N_DP, slice_width).astype(jnp.float32)
    weight_split = w_out[expert_id].reshape(N_DP, slice_width, D).astype(jnp.float32)
    partials = jnp.einsum("bjs,jsd->jbd", hidden_split, weight_split).astype(jnp.bfloat16)
    partials = lax.optimization_barrier(partials).astype(jnp.float32)
    return jnp.sum(partials, axis=0)


def reference(tokens, task_ids, routing, gate_weight, w_in, w_out):
    token_blocks = tokens.reshape(BLOCKS, BLK, D)

    def per_block(inputs):
        block_rows, task_id, route_pair = inputs
        logits = jnp.dot(block_rows, gate_weight, preferred_element_type=jnp.float32).reshape(BLK, TASKS, EXPERTS)
        task_logits = lax.dynamic_index_in_dim(logits, task_id, 1, keepdims=False)
        logit_first = task_logits[:, route_pair[0]]
        logit_second = task_logits[:, route_pair[1]]
        gate_first = jax.nn.sigmoid(logit_first - logit_second)
        gate_second = jax.nn.sigmoid(logit_second - logit_first)
        first_sum = expert_output(block_rows, route_pair[0], w_in, w_out)
        second_sum = expert_output(block_rows, route_pair[1], w_in, w_out)
        gated_first = (gate_first[:, None] * first_sum).astype(jnp.bfloat16)
        gated_second = (gate_second[:, None] * second_sum).astype(jnp.bfloat16)
        return (gated_first.astype(jnp.float32) + gated_second.astype(jnp.float32)).astype(jnp.bfloat16)

    mixed = lax.map(per_block, (token_blocks, task_ids, routing))
    return mixed.reshape(TOKENS, D)
```

```python
import functools

import jax
import jax.numpy as jnp
from jax import lax
from jax.experimental import pallas as pl
from jax.experimental.pallas import tpu as pltpu
from jax.sharding import PartitionSpec as P

BLK = 128
ROWS = 16
TILE = 512
MESH = pl.DeviceIdType.MESH
START = {"y": 5.0, "x": 9.0, "relay": 13.2, "expert": 14.4, "back": 16.7, "gate": 20.8, "share": 25.0, "out": 30.0}
STEP = {"y": 2.8, "x": 2.8, "relay": 2.8, "expert": 2.8, "back": 3.5, "gate": 3.5, "share": 3.5, "out": 3.5}


def gelu(x):
    return 0.5 * x * (1.0 + jnp.tanh(0.7978845608028654 * (x + 0.044715 * (x * x * x))))


def kernel(
    n, n_dp, capacity,
    routing, tasks, tokens_hbm, gate_hbm, w_in_hbm, w_out_hbm, out_hbm,
    tokens, gate_weight, w_in, w_out, line, picked, given, cols, hidden, acc, pout, pin, xs, xr, gated,
    weights, shares, landed, result,
    ld, zs, zr, ys, yr, x_s, x_r, b_s, b_r, p_s, p_r, q_s, q_r, v_s, v_r, u_s, u_r, o_s,
):
    d_model = tokens.shape[1]
    parts = BLK // ROWS
    chips = n_dp // 2
    reach = n // 2
    wide = capacity * ROWS
    me = lax.axis_index("expert")
    my_dp = lax.axis_index("dp")
    my_x, my_core = my_dp // 2, my_dp % 2
    at, row = me // 2, me % 2
    other = me + 1 - 2 * row
    pair = {"expert": other}
    sibling = {"dp": my_x * 2 + 1 - my_core}

    def peer(j):
        return {"expert": ((at + j) % reach) * 2 + row}

    def chip(k):
        return {"dp": ((my_x + k) % chips) * 2 + my_core}

    loads = [
        pltpu.make_async_copy(tokens_hbm, tokens, ld.at[0]),
        pltpu.make_async_copy(w_in_hbm.at[0], w_in, ld.at[1]),
        pltpu.make_async_copy(w_out_hbm.at[0], w_out, ld.at[2]),
        pltpu.make_async_copy(gate_hbm, gate_weight, ld.at[3]),
    ]
    for load in loads:
        load.start()

    barrier = pltpu.get_barrier_semaphore()
    partners = [peer(j) for j in range(1, reach)] + [pair, sibling] + [chip(k) for k in range(1, chips)]
    for partner in partners:
        pl.semaphore_signal(barrier, inc=1, device_id=partner, device_id_type=MESH)
    pl.semaphore_wait(barrier, len(partners))

    def remote(src, dst, send, recv, target):
        return pltpu.make_async_remote_copy(
            src_ref=src, dst_ref=dst, send_sem=send, recv_sem=recv,
            device_id=target, device_id_type=MESH,
        )

    sent = []

    def go(copy):
        copy.start()
        sent.append(copy)

    def span(c):
        return slice(c * ROWS, (c + 1) * ROWS)

    def z_copy(c, j):
        return remote(
            tokens.at[pl.ds(c * ROWS, ROWS)], line[c].at[reach - j], zs.at[c, j], zr.at[c, reach - j], peer(j)
        )

    loads[0].wait()
    for c in range(parts):
        for j in range(1, reach):
            go(z_copy(c, j))

    def ranks(expert):
        hits, before, count = [], [], 0
        for m in range(n):
            hit = jnp.where(routing[0, m] == expert, 1, 0) + jnp.where(routing[1, m] == expert, 1, 0)
            hits.append(hit)
            before.append(count)
            count = count + hit
        return hits, before

    def rel(m):
        return (m // 2 + reach - at) % reach

    hits, before = ranks(me)
    theirs, theirs_before = ranks(other)

    def within(taken, member):
        order, count = [], 0
        for m in range(n):
            keep = taken[m] * jnp.where(m % 2 == member, 1, 0)
            order.append((keep, count))
            count = count + keep
        return order

    give = within(theirs, row)
    take = within(hits, 1 - row)
    give_at, slot_at, slot_other, slot_task, slot_valid = [], [], [], [], []
    for slot in range(capacity):
        place = 0
        for m in range(n):
            keep, count = give[m]
            place = place + keep * jnp.where(count == slot, 1, 0) * rel(m)
        give_at.append(jnp.clip(place, 0, reach - 1))
        place, against, task, valid = 0, 0, 0, 0
        for m in range(n):
            here = hits[m] * jnp.where(before[m] == slot, 1, 0)
            near = jnp.where(m % 2 == row, 1, 0)
            place = place + here * (near * rel(m) + (1 - near) * (reach + take[m][1]))
            against = against + here * (routing[0, m] + routing[1, m] - me)
            task = task + here * tasks[m]
            valid = valid + here
        slot_at.append(jnp.clip(place, 0, reach + capacity - 1))
        slot_other.append(against)
        slot_task.append(task)
        slot_valid.append(valid)

    def slot_of(taken, earlier, j, base):
        e = ((at + j) % reach) * 2 + row
        place = 0
        for m in range(n):
            here = taken[m] * jnp.where(m == e, 1, 0)
            place = place + here * (base + earlier[m] - 2 * capacity)
        return jnp.clip(place + 2 * capacity, 0, 2 * capacity)

    mine_for = [slot_of(hits, before, j, 0) for j in range(reach)]
    pair_for = [slot_of(theirs, theirs_before, j, capacity) for j in range(reach)]

    def y_copy(c):
        return remote(picked.at[c], given.at[c], ys.at[c], yr.at[c], pair)

    def x_copy(c, k):
        return remote(
            cols.at[c, 0, 0], cols.at[c, chips - k, 0], x_s.at[c, k], x_r.at[c, chips - k], chip(k)
        )

    def x_recv(c, k):
        return remote(
            cols.at[c, 0, 0], cols.at[c, k, 0], x_s.at[c, chips - k], x_r.at[c, k], chip(chips - k)
        )

    def b_copy(c, k):
        return remote(cols.at[c, k, 0], cols.at[c, k, 1], b_s.at[c, k], b_r.at[c, k], sibling)

    def p_copy(c, k):
        return remote(pout.at[c, k], pin.at[c, k], p_s.at[c, k], p_r.at[c, k], sibling)

    def q_copy(c, k):
        return remote(xs.at[c, k], xr.at[c, chips - k], q_s.at[c, k], q_r.at[c, chips - k], chip(k))

    def q_recv(c, k):
        return remote(xs.at[c, chips - k], xr.at[c, k], q_s.at[c, chips - k], q_r.at[c, k], chip(chips - k))

    def v_copy(c):
        return remote(
            gated[c].at[pl.ds(0, capacity)], gated[c].at[pl.ds(capacity, capacity)], v_s.at[c], v_r.at[c], pair
        )

    def u_copy(c, j):
        return remote(shares.at[c, j], landed.at[c, reach - j], u_s.at[c, j], u_r.at[c, reach - j], peer(j))

    def y_stage(c):
        for j in range(1, reach):
            z_copy(c, reach - j).wait_recv()
        line[c][0] = tokens[span(c), :]
        for slot in range(capacity):
            picked[c, slot] = line[c][give_at[slot]]
        go(y_copy(c))

    def x_stage(c):
        y_copy(c).wait_recv()
        line[c][reach:] = given[c]
        for slot in range(capacity):
            cols[c, 0, 0, slot * ROWS : (slot + 1) * ROWS, :] = line[c][slot_at[slot]]
        for k in range(1, chips):
            go(x_copy(c, k))
        go(b_copy(c, 0))
        if c == 0:
            loads[3].wait()
        logits = lax.dot_general(
            cols[c, 0, 0], gate_weight[...], (((1,), (1,)), ((), ())), preferred_element_type=jnp.float32
        )
        column = lax.broadcasted_iota(jnp.int32, (ROWS, logits.shape[1]), 1)
        for slot in range(capacity):
            own = slot_task[slot] * n + me
            against = slot_task[slot] * n + slot_other[slot]
            sign = jnp.where(column == own, 1.0, 0.0) - jnp.where(column == against, 1.0, 0.0)
            gap = jnp.sum(logits[slot * ROWS : (slot + 1) * ROWS] * sign, axis=1, keepdims=True)
            gate = jax.nn.sigmoid(gap) * slot_valid[slot].astype(jnp.float32)
            weights[c, slot * ROWS : (slot + 1) * ROWS, :] = jnp.broadcast_to(gate, (ROWS, 128))

    def relay_stage(c):
        for k in range(1, chips):
            x_recv(c, k).wait_recv()
            go(b_copy(c, k))

    def expert_stage(c):
        if c == 0:
            loads[1].wait()
            loads[2].wait()
        for k in range(chips):
            b_copy(c, k).wait_recv()
        lhs = cols.at[c]
        tall = chips * 2 * wide

        @pl.loop(0, w_in.shape[1] // TILE)
        def _(t):
            where = pl.ds(pl.multiple_of(t * TILE, TILE), TILE)
            x = lhs[...].reshape(tall, d_model)
            y = jnp.dot(x, w_in[:, where], preferred_element_type=jnp.float32)
            hidden[:, where] = gelu(y).astype(jnp.bfloat16)

        @pl.loop(0, d_model // TILE)
        def _(t):
            where = pl.ds(pl.multiple_of(t * TILE, TILE), TILE)
            y = jnp.dot(hidden[...], w_out[:, where], preferred_element_type=jnp.float32)
            for k in range(chips):
                acc[c, k, :, where] = y[2 * k * wide : (2 * k + 1) * wide]
                pout[c, k, :, where] = y[(2 * k + 1) * wide : (2 * k + 2) * wide].astype(jnp.bfloat16)

        for k in range(chips - 1, -1, -1):
            go(p_copy(c, k))

    def back_stage(c):
        for k in range(1, chips):
            p_copy(c, k).wait_recv()
            xs[c, k] = (acc[c, k] + pin[c, k].astype(jnp.float32)).astype(jnp.bfloat16)
            go(q_copy(c, k))

    def gate_stage(c):
        p_copy(c, 0).wait_recv()
        for k in range(1, chips):
            q_recv(c, k).wait_recv()
        for slot in range(capacity):
            rows = slice(slot * ROWS, (slot + 1) * ROWS)
            total = acc[c, 0, rows, :] + pin[c, 0, rows, :].astype(jnp.float32)
            for k in range(1, chips):
                total = total + xr[c, k, rows, :].astype(jnp.float32)
            gated[c][slot] = (weights[c, rows, :1] * total).astype(jnp.bfloat16)
        gated[c][2 * capacity] = jnp.zeros((ROWS, d_model), jnp.bfloat16)
        go(v_copy(c))

    def share(c, j):
        return gated[c][mine_for[j]].astype(jnp.float32) + gated[c][pair_for[j]].astype(jnp.float32)

    def share_stage(c):
        v_copy(c).wait_recv()
        for j in range(1, reach):
            shares[c, j] = share(c, j).astype(jnp.bfloat16)
            go(u_copy(c, j))

    def out_copy(c):
        return pltpu.make_async_copy(result.at[pl.ds(c * ROWS, ROWS)], out_hbm.at[pl.ds(c * ROWS, ROWS)], o_s.at[c])

    def out_stage(c):
        total = share(c, 0)
        for j in range(1, reach):
            u_copy(c, reach - j).wait_recv()
            total = total + landed[c, j].astype(jnp.float32)
        result[span(c), :] = total.astype(jnp.bfloat16)
        out_copy(c).start()

    stages = {
        "y": y_stage, "x": x_stage, "relay": relay_stage, "expert": expert_stage,
        "back": back_stage, "gate": gate_stage, "share": share_stage, "out": out_stage,
    }
    plan = []
    for c in range(parts):
        for name in stages:
            plan.append((START[name] + STEP[name] * c, len(plan), name, c))
    for _, _, name, c in sorted(plan):
        stages[name](c)
    for copy in sent:
        copy.wait_send()
    for c in range(parts):
        out_copy(c).wait()


def shards(tokens, task_ids, routing, gate_weight, w_in, w_out):
    n = lax.axis_size("expert")
    n_dp = lax.axis_size("dp")
    d_model = tokens.shape[1]
    capacity = 2 * (tokens.shape[0] // BLK) + 1
    chips, reach = n_dp // 2, n // 2
    parts = BLK // ROWS
    wide = capacity * ROWS
    bf16 = jnp.bfloat16
    dma = pltpu.SemaphoreType.DMA
    smem = pl.BlockSpec(memory_space=pltpu.SMEM)
    hbm = pl.BlockSpec(memory_space=pl.ANY)
    return pl.pallas_call(
        functools.partial(kernel, n, n_dp, capacity),
        out_shape=jax.ShapeDtypeStruct(tokens.shape, bf16),
        in_specs=[smem, smem, hbm, hbm, hbm, hbm],
        out_specs=hbm,
        scratch_shapes=[
            pltpu.VMEM(tokens.shape, bf16),
            pltpu.VMEM(gate_weight.shape[::-1], bf16),
            pltpu.VMEM(w_in.shape[1:], bf16),
            pltpu.VMEM(w_out.shape[1:], bf16),
            [pltpu.VMEM((reach + capacity, ROWS, d_model), bf16) for _ in range(parts)],
            pltpu.VMEM((parts, capacity, ROWS, d_model), bf16),
            pltpu.VMEM((parts, capacity, ROWS, d_model), bf16),
            pltpu.VMEM((parts, chips, 2, wide, d_model), bf16),
            pltpu.VMEM((chips * 2 * wide, w_in.shape[2]), bf16),
            pltpu.VMEM((parts, chips, wide, d_model), jnp.float32),
            pltpu.VMEM((parts, chips, wide, d_model), bf16),
            pltpu.VMEM((parts, chips, wide, d_model), bf16),
            pltpu.VMEM((parts, chips, wide, d_model), bf16),
            pltpu.VMEM((parts, chips, wide, d_model), bf16),
            [pltpu.VMEM((2 * capacity + 1, ROWS, d_model), bf16) for _ in range(parts)],
            pltpu.VMEM((parts, wide, 128), jnp.float32),
            pltpu.VMEM((parts, reach, ROWS, d_model), bf16),
            pltpu.VMEM((parts, reach, ROWS, d_model), bf16),
            pltpu.VMEM(tokens.shape, bf16),
            dma((4,)),
            dma((parts, reach)),
            dma((parts, reach)),
            dma((parts,)),
            dma((parts,)),
            dma((parts, chips)),
            dma((parts, chips)),
            dma((parts, chips)),
            dma((parts, chips)),
            dma((parts, chips)),
            dma((parts, chips)),
            dma((parts, chips)),
            dma((parts, chips)),
            dma((parts,)),
            dma((parts,)),
            dma((parts, reach)),
            dma((parts, reach)),
            dma((parts,)),
        ],
        compiler_params=pltpu.CompilerParams(
            collective_id=0, has_side_effects=True, vmem_limit_bytes=64 * 1024 * 1024 - 65536
        ),
    )(routing.T, task_ids, tokens, gate_weight.T, w_in, w_out)


def solution(mesh):
    placed = (
        P(("dp", "expert"), None),
        P("dp"),
        P("dp", None),
        P(),
        P("expert", None, "dp"),
        P("expert", "dp", None),
    )
    return jax.shard_map(
        shards, mesh=mesh, in_specs=placed, out_specs=P(("dp", "expert"), None), check_vma=False
    )
```

```python
import functools

import jax
import jax.numpy as jnp
from jax import lax
from jax.experimental import pallas as pl
from jax.experimental.pallas import tpu as pltpu
from jax.sharding import PartitionSpec as P

BLK = 128
ROWS = 16
PIECES = 2
MESH = pl.DeviceIdType.MESH
LAGS = {
    "z": -7.0, "zf": -2.0, "y": -0.8, "x": 1.2, "relay": 2.7, "expert": 3.4, "back": 4.6, "gate": 6.4,
    "share": 8.5, "sf": 10.5, "out": 13.5,
}


def gelu(x):
    return 0.5 * x * (1.0 + jnp.tanh(0.7978845608028654 * (x + 0.044715 * (x * x * x))))


def kernel(
    n, n_dp, capacity, pieces,
    routing_hbm, tasks_hbm, tokens_hbm, gate_hbm, w_in_hbm, w_out_hbm, out_hbm,
    routing, tasks, tokens, gate_weight, w_in, w_out, line, picked, given, cols, hidden, acc, pout, pin, xs, xr,
    gated, weights, shares, passed, landed, result,
    ld, far, zs, zr, ys, yr, x_s, x_r, b_s, b_r, p_s, p_r, q_s, q_r, v_s, v_r, u_s, u_r, f_r, o_s,
):
    d_model = tokens.shape[1]
    width = d_model // pieces
    parts = BLK // ROWS
    chips = n_dp // 2
    reach = n // 2
    wide = capacity * ROWS
    hops = min(2, reach - 1)
    me = lax.axis_index("expert")
    my_dp = lax.axis_index("dp")
    my_x, my_core = my_dp // 2, my_dp % 2
    at, row = me // 2, me % 2
    other = me + 1 - 2 * row
    pair = {"expert": other}
    sibling = {"dp": my_x * 2 + 1 - my_core}

    def along(way, hop):
        return {"expert": (at + hop if way == 0 else at - hop) * 2 + row}

    def ahead(way, hop):
        return at + hop < reach if way == 0 else at >= hop

    def behind(way, hop):
        return ahead(1 - way, hop)

    def chip(k):
        return {"dp": ((my_x + k) % chips) * 2 + my_core}

    loads = [
        pltpu.make_async_copy(tokens_hbm, tokens, ld.at[0]),
        pltpu.make_async_copy(routing_hbm, routing, ld.at[4]),
        pltpu.make_async_copy(tasks_hbm, tasks, ld.at[5]),
        pltpu.make_async_copy(gate_hbm, gate_weight, ld.at[3]),
        pltpu.make_async_copy(w_in_hbm.at[0], w_in, ld.at[1]),
        pltpu.make_async_copy(w_out_hbm.at[0], w_out, ld.at[2]),
    ]
    for load in loads[:3]:
        load.start()

    barrier = pltpu.get_barrier_semaphore()
    for way in range(2):

        @pl.when(ahead(way, 1))
        def _():
            pl.semaphore_signal(barrier, inc=1, device_id=along(way, 1), device_id_type=MESH)

    partners = [pair, sibling] + [chip(k) for k in range(1, chips)]
    for partner in partners:
        pl.semaphore_signal(barrier, inc=1, device_id=partner, device_id_type=MESH)
    for load in loads[3:]:
        load.start()
    ends = jnp.where(at == 0, 1, 0) + jnp.where(at == reach - 1, 1, 0)
    pl.semaphore_wait(barrier, len(partners) + 2 - ends)

    def remote(src, dst, send, recv, target):
        return pltpu.make_async_remote_copy(
            src_ref=src, dst_ref=dst, send_sem=send, recv_sem=recv,
            device_id=target, device_id_type=MESH,
        )

    sent = []

    def go(copy):
        copy.start()
        sent.append((None, copy))

    def go_if(cond, make):
        @pl.when(cond)
        def _():
            make().start()

        sent.append((cond, make))

    def wait_if(cond, make):
        @pl.when(cond)
        def _():
            make().wait_recv()

    def where_of(i):
        c, s = i // pieces, i % pieces
        return c, s, slice(c * ROWS, (c + 1) * ROWS), slice(s * width, (s + 1) * width)

    def place(way, d):
        return reach - d if way == 0 else d

    def z_copy(i, way, hop):
        c, s, _, _ = where_of(i)
        src = tokens.at[pl.ds(c * ROWS, ROWS), pl.ds(s * width, width)]
        return remote(src, line[i].at[place(way, hop)], zs.at[i, way, hop], zr.at[i, way, hop], along(way, hop))

    def zf_copy(i, way, d):
        return remote(
            line[i].at[place(way, d)], line[i].at[place(way, d + 1)],
            zs.at[i, way, d + 1], zr.at[i, way, d + 1], along(way, 1),
        )

    def z_wait(i, d):
        for way in range(2):
            wait_if(behind(way, d), lambda: z_copy(i, way, 1) if d == 1 else zf_copy(i, way, d - 1))

    def z_stage(i, which):
        for hop in which:
            for way in range(2):
                go_if(ahead(way, hop), functools.partial(z_copy, i, way, hop))

    def zf_stage(i):
        for d in range(2, reach - 1):
            z_wait(i, d)
            for way in range(2):
                go_if(jnp.logical_and(behind(way, d), ahead(way, 1)), functools.partial(zf_copy, i, way, d))

    loads[0].wait()
    z_stage(0, [1])
    if hops > 1:
        for way in range(2):

            @pl.when(jnp.logical_and(ahead(way, 1), behind(way, 1)))
            def _():
                pl.semaphore_signal(far.at[way], inc=1, device_id=along(way, 1), device_id_type=MESH)

        for way in range(2):

            @pl.when(behind(way, 2))
            def _():
                pl.semaphore_wait(far.at[way], 1)

        z_stage(0, [2])
    every = list(range(1, hops + 1))
    ready = max(1, int(-LAGS["z"]) - 2)
    for i in range(1, ready):
        z_stage(i, every)

    loads[1].wait()
    loads[2].wait()

    def ranks(expert):
        hits, before, count = [], [], 0
        for m in range(n):
            hit = jnp.where(routing[0, m] == expert, 1, 0) + jnp.where(routing[1, m] == expert, 1, 0)
            hits.append(hit)
            before.append(count)
            count = count + hit
        return hits, before

    def rel(m):
        return (m // 2 + reach - at) % reach

    hits, before = ranks(me)
    theirs, theirs_before = ranks(other)

    def within(taken, member):
        order, count = [], 0
        for m in range(n):
            keep = taken[m] * jnp.where(m % 2 == member, 1, 0)
            order.append((keep, count))
            count = count + keep
        return order

    give = within(theirs, row)
    take = within(hits, 1 - row)
    give_at, slot_at, slot_other, slot_task, slot_valid = [], [], [], [], []
    for slot in range(capacity):
        spot = 0
        for m in range(n):
            keep, count = give[m]
            spot = spot + keep * jnp.where(count == slot, 1, 0) * rel(m)
        give_at.append(jnp.clip(spot, 0, reach - 1))
        spot, against, task, valid = 0, 0, 0, 0
        for m in range(n):
            here = hits[m] * jnp.where(before[m] == slot, 1, 0)
            near = jnp.where(m % 2 == row, 1, 0)
            spot = spot + here * (near * rel(m) + (1 - near) * (reach + take[m][1]))
            against = against + here * (routing[0, m] + routing[1, m] - me)
            task = task + here * tasks[m]
            valid = valid + here
        slot_at.append(jnp.clip(spot, 0, reach + capacity - 1))
        slot_other.append(against)
        slot_task.append(task)
        slot_valid.append(valid)

    def slot_of(taken, earlier, j, base):
        e = ((at + j) % reach) * 2 + row
        spot = 0
        for m in range(n):
            here = taken[m] * jnp.where(m == e, 1, 0)
            spot = spot + here * (base + earlier[m] - 2 * capacity)
        return jnp.clip(spot + 2 * capacity, 0, 2 * capacity)

    mine_for = [slot_of(hits, before, j, 0) for j in range(reach)]
    pair_for = [slot_of(theirs, theirs_before, j, capacity) for j in range(reach)]

    def y_copy(i):
        return remote(picked.at[i], given.at[i], ys.at[i], yr.at[i], pair)

    def x_copy(i, k):
        return remote(
            cols.at[i, 0, 0], cols.at[i, chips - k, 0], x_s.at[i, k], x_r.at[i, chips - k], chip(k)
        )

    def x_recv(i, k):
        return remote(
            cols.at[i, 0, 0], cols.at[i, k, 0], x_s.at[i, chips - k], x_r.at[i, k], chip(chips - k)
        )

    def b_copy(i, k):
        return remote(cols.at[i, k, 0], cols.at[i, k, 1], b_s.at[i, k], b_r.at[i, k], sibling)

    def p_copy(i, k):
        return remote(pout.at[i, k], pin.at[i, k], p_s.at[i, k], p_r.at[i, k], sibling)

    def q_copy(i, k):
        return remote(xs.at[i, k], xr.at[i, chips - k], q_s.at[i, k], q_r.at[i, chips - k], chip(k))

    def q_recv(i, k):
        return remote(xs.at[i, chips - k], xr.at[i, k], q_s.at[i, chips - k], q_r.at[i, k], chip(chips - k))

    def v_copy(i):
        return remote(
            gated[i].at[pl.ds(0, capacity)], gated[i].at[pl.ds(capacity, capacity)], v_s.at[i], v_r.at[i], pair
        )

    def u_copy(i, way, j):
        if j > hops:
            return remote(
                shares.at[i, way, j], passed.at[i, way, j - 1],
                u_s.at[i, way, j], f_r.at[i, way, j - 1], along(way, 1),
            )
        return remote(
            shares.at[i, way, j], landed.at[i, way, j], u_s.at[i, way, j], u_r.at[i, way, j], along(way, j)
        )

    def y_stage(i):
        c, s, rows, part = where_of(i)
        for d in sorted({1, reach - 1}):
            z_wait(i, d)
        line[i][0] = tokens[rows, part]
        for slot in range(capacity):
            picked[i, slot] = line[i][give_at[slot]]
        go(y_copy(i))

    def x_stage(i):
        y_copy(i).wait_recv()
        line[i][reach:] = given[i]
        for slot in range(capacity):
            cols[i, 0, 0, slot * ROWS : (slot + 1) * ROWS, :] = line[i][slot_at[slot]]
        for k in range(1, chips):
            go(x_copy(i, k))
        go(b_copy(i, 0))
        if i == 0:
            loads[3].wait()
        if i % pieces == pieces - 1:
            gates(i // pieces)

    def whole(c, *index):
        return jnp.concatenate([cols[(c * pieces + s, *index)] for s in range(pieces)], axis=-1)

    def gates(c):
        logits = lax.dot_general(
            whole(c, 0, 0), gate_weight[...], (((1,), (1,)), ((), ())), preferred_element_type=jnp.float32
        )
        column = lax.broadcasted_iota(jnp.int32, (ROWS, logits.shape[1]), 1)
        for slot in range(capacity):
            own = slot_task[slot] * n + me
            against = slot_task[slot] * n + slot_other[slot]
            sign = jnp.where(column == own, 1.0, 0.0) - jnp.where(column == against, 1.0, 0.0)
            gap = jnp.sum(logits[slot * ROWS : (slot + 1) * ROWS] * sign, axis=1, keepdims=True)
            gate = jax.nn.sigmoid(gap) * slot_valid[slot].astype(jnp.float32)
            weights[c, slot * ROWS : (slot + 1) * ROWS, :] = jnp.broadcast_to(gate, (ROWS, 128))

    def relay_stage(i):
        for k in range(1, chips):
            x_recv(i, k).wait_recv()
            go(b_copy(i, k))

    def expert_stage(i):
        c = i // pieces
        if c == 0:
            loads[4].wait()
            loads[5].wait()
        for s in range(pieces):
            for k in range(chips):
                b_copy(c * pieces + s, k).wait_recv()
        tall = chips * 2 * wide
        x = whole(c).reshape(tall, d_model)
        y = jnp.dot(x, w_in[...], preferred_element_type=jnp.float32)
        hidden[...] = gelu(y).astype(jnp.bfloat16)
        for s in range(pieces):
            u = c * pieces + s
            y = jnp.dot(hidden[...], w_out[:, s * width : (s + 1) * width], preferred_element_type=jnp.float32)
            for k in range(chips - 1, -1, -1):
                acc[u, k] = y[2 * k * wide : (2 * k + 1) * wide]
                pout[u, k] = y[(2 * k + 1) * wide : (2 * k + 2) * wide].astype(jnp.bfloat16)
                go(p_copy(u, k))

    def back_stage(i):
        for k in range(1, chips):
            p_copy(i, k).wait_recv()
            xs[i, k] = (acc[i, k] + pin[i, k].astype(jnp.float32)).astype(jnp.bfloat16)
            go(q_copy(i, k))

    def gate_stage(i):
        p_copy(i, 0).wait_recv()
        for k in range(1, chips):
            q_recv(i, k).wait_recv()
        for slot in range(capacity):
            rows = slice(slot * ROWS, (slot + 1) * ROWS)
            total = acc[i, 0, rows, :] + pin[i, 0, rows, :].astype(jnp.float32)
            for k in range(1, chips):
                total = total + xr[i, k, rows, :].astype(jnp.float32)
            gated[i][slot] = (weights[i // pieces, rows, :1] * total).astype(jnp.bfloat16)
        gated[i][2 * capacity] = jnp.zeros((ROWS, width), jnp.bfloat16)
        go(v_copy(i))

    def share(i, j):
        return gated[i][mine_for[j]].astype(jnp.float32) + gated[i][pair_for[j]].astype(jnp.float32)

    def share_stage(i):
        v_copy(i).wait_recv()
        for j in range(reach - 1, 0, -1):
            for way in range(2):
                shares[i, way, j] = share(i, j if way == 0 else reach - j).astype(jnp.bfloat16)
                cond = ahead(way, j)
                if j >= hops and j > 1:
                    cond = jnp.logical_and(cond, jnp.logical_not(behind(way, 1)))
                go_if(cond, functools.partial(u_copy, i, way, j))

    def sf_stage(i):
        for j in range(reach - 2, 1, -1):
            for way in range(2):
                cond = jnp.logical_and(ahead(way, j), behind(way, 1))

                @pl.when(cond)
                def _():
                    u_copy(i, way, j + 1).wait_recv()
                    total = shares[i, way, j].astype(jnp.float32) + passed[i, way, j].astype(jnp.float32)
                    shares[i, way, j] = total.astype(jnp.bfloat16)

                go_if(cond, functools.partial(u_copy, i, way, j))

    def out_copy(i):
        c, s, _, _ = where_of(i)
        spot = (pl.ds(c * ROWS, ROWS), pl.ds(s * width, width))
        return pltpu.make_async_copy(result.at[spot], out_hbm.at[spot], o_s.at[i])

    def out_stage(i):
        c, s, rows, part = where_of(i)
        total = share(i, 0)
        for j in range(1, hops + 1):
            for way in range(2):
                wait_if(behind(way, j), functools.partial(u_copy, i, way, j))
                total = total + jnp.where(behind(way, j), landed[i, way, j].astype(jnp.float32), 0.0)
        result[rows, part] = total.astype(jnp.bfloat16)
        out_copy(i).start()

    stages = {
        "z": lambda i: z_stage(i, every), "zf": zf_stage, "y": y_stage, "x": x_stage, "relay": relay_stage,
        "expert": expert_stage, "back": back_stage, "gate": gate_stage, "share": share_stage, "sf": sf_stage,
        "out": out_stage,
    }
    plan = []
    for i in range(parts * pieces):
        for name in stages:
            if name == "z" and i < ready:
                continue
            if name == "expert" and i % pieces < pieces - 1:
                continue
            plan.append((LAGS[name] + i, len(plan), name, i))
    for _, _, name, i in sorted(plan):
        stages[name](i)
    for cond, copy in sent:
        if cond is None:
            copy.wait_send()
        else:

            @pl.when(cond)
            def _():
                copy().wait_send()

    for i in range(parts * pieces):
        out_copy(i).wait()


def shards(tokens, task_ids, routing, gate_weight, w_in, w_out):
    n = lax.axis_size("expert")
    n_dp = lax.axis_size("dp")
    d_model = tokens.shape[1]
    capacity = 2 * (tokens.shape[0] // BLK) + 1
    chips, reach = n_dp // 2, n // 2
    parts = BLK // ROWS
    pieces = PIECES if reach <= 4 else 1
    units, width = parts * pieces, d_model // pieces
    wide = capacity * ROWS
    bf16 = jnp.bfloat16
    dma = pltpu.SemaphoreType.DMA
    hbm = pl.BlockSpec(memory_space=pl.ANY)

    def vmem(*shape):
        return pltpu.VMEM(shape, bf16)

    return pl.pallas_call(
        functools.partial(kernel, n, n_dp, capacity, pieces),
        out_shape=jax.ShapeDtypeStruct(tokens.shape, bf16),
        in_specs=[hbm] * 6,
        out_specs=hbm,
        scratch_shapes=[
            pltpu.SMEM(routing.shape[::-1], jnp.int32),
            pltpu.SMEM(task_ids.shape, jnp.int32),
            vmem(*tokens.shape),
            vmem(*gate_weight.shape[::-1]),
            vmem(*w_in.shape[1:]),
            vmem(*w_out.shape[1:]),
            [vmem(reach + capacity, ROWS, width) for _ in range(units)],
            vmem(units, capacity, ROWS, width),
            vmem(units, capacity, ROWS, width),
            vmem(units, chips, 2, wide, width),
            vmem(chips * 2 * wide, w_in.shape[2]),
            pltpu.VMEM((units, chips, wide, width), jnp.float32),
            vmem(units, chips, wide, width),
            vmem(units, chips, wide, width),
            vmem(units, chips, wide, width),
            vmem(units, chips, wide, width),
            [vmem(2 * capacity + 1, ROWS, width) for _ in range(units)],
            pltpu.VMEM((parts, wide, 128), jnp.float32),
            vmem(units, 2, reach, ROWS, width),
            vmem(units, 2, reach, ROWS, width),
            vmem(units, 2, 3, ROWS, width),
            vmem(*tokens.shape),
            dma((6,)),
            pltpu.SemaphoreType.REGULAR((2,)),
            dma((units, 2, reach)),
            dma((units, 2, reach)),
            dma((units,)),
            dma((units,)),
            dma((units, chips)),
            dma((units, chips)),
            dma((units, chips)),
            dma((units, chips)),
            dma((units, chips)),
            dma((units, chips)),
            dma((units, chips)),
            dma((units, chips)),
            dma((units,)),
            dma((units,)),
            dma((units, 2, reach)),
            dma((units, 2, 3)),
            dma((units, 2, reach)),
            dma((units,)),
        ],
        compiler_params=pltpu.CompilerParams(
            collective_id=0, has_side_effects=True, vmem_limit_bytes=64 * 1024 * 1024 - 65536
        ),
    )(routing.T, task_ids, tokens, gate_weight.T, w_in, w_out)


def solution(mesh):
    placed = (
        P(("dp", "expert"), None),
        P("dp"),
        P("dp", None),
        P(),
        P("expert", None, "dp"),
        P("expert", "dp", None),
    )
    return jax.shard_map(
        shards, mesh=mesh, in_specs=placed, out_specs=P(("dp", "expert"), None), check_vma=False
    )
```

```python
import functools

import jax
import jax.numpy as jnp
from jax import lax
from jax.experimental import pallas as pl
from jax.experimental.pallas import tpu as pltpu
from jax.sharding import PartitionSpec as P

BLK = 128
ROWS = 16
MESH = pl.DeviceIdType.MESH
LAGS = {"y": 0, "x": 1.25, "relay": 2.5, "expert": 2.9, "back": 3.6, "gate": 4.9, "share": 6.2, "out": 7.9}


def gelu(x):
    return 0.5 * x * (1.0 + jnp.tanh(0.7978845608028654 * (x + 0.044715 * (x * x * x))))


def kernel(
    n, n_dp, capacity,
    routing_hbm, tasks_hbm, tokens_hbm, gate_hbm, w_in_hbm, w_out_hbm, out_hbm,
    routing, tasks, tokens, gate_weight, w_in, w_out, line, picked, given, cols, hidden, acc, pout, pin, xs, xr, gated,
    weights, shares, landed, result,
    ld, zs, zr, ys, yr, x_s, x_r, b_s, b_r, p_s, p_r, q_s, q_r, v_s, v_r, u_s, u_r, o_s,
):
    d_model = tokens.shape[1]
    parts = BLK // ROWS
    chips = n_dp // 2
    reach = n // 2
    wide = capacity * ROWS
    me = lax.axis_index("expert")
    my_dp = lax.axis_index("dp")
    my_x, my_core = my_dp // 2, my_dp % 2
    at, row = me // 2, me % 2
    other = me + 1 - 2 * row
    pair = {"expert": other}
    sibling = {"dp": my_x * 2 + 1 - my_core}

    def peer(j):
        return {"expert": ((at + j) % reach) * 2 + row}

    def chip(k):
        return {"dp": ((my_x + k) % chips) * 2 + my_core}

    loads = [
        pltpu.make_async_copy(tokens_hbm, tokens, ld.at[0]),
        pltpu.make_async_copy(w_in_hbm.at[0], w_in, ld.at[1]),
        pltpu.make_async_copy(w_out_hbm.at[0], w_out, ld.at[2]),
        pltpu.make_async_copy(gate_hbm, gate_weight, ld.at[3]),
        pltpu.make_async_copy(routing_hbm, routing, ld.at[4]),
        pltpu.make_async_copy(tasks_hbm, tasks, ld.at[5]),
    ]
    for load in [loads[0]] + loads[4:] + loads[1:4]:
        load.start()

    barrier = pltpu.get_barrier_semaphore()
    partners = [peer(j) for j in range(1, reach)] + [pair, sibling] + [chip(k) for k in range(1, chips)]
    for partner in partners:
        pl.semaphore_signal(barrier, inc=1, device_id=partner, device_id_type=MESH)
    pl.semaphore_wait(barrier, len(partners))

    def remote(src, dst, send, recv, target):
        return pltpu.make_async_remote_copy(
            src_ref=src, dst_ref=dst, send_sem=send, recv_sem=recv,
            device_id=target, device_id_type=MESH,
        )

    sent = []

    def go(copy):
        copy.start()
        sent.append(copy)

    def span(c):
        return slice(c * ROWS, (c + 1) * ROWS)

    def z_copy(c, j):
        return remote(
            tokens.at[pl.ds(c * ROWS, ROWS)], line[c].at[reach - j], zs.at[c, j], zr.at[c, reach - j], peer(j)
        )

    loads[0].wait()
    for c in range(parts):
        for j in range(1, reach):
            go(z_copy(c, j))

    loads[4].wait()
    loads[5].wait()

    def ranks(expert):
        hits, before, count = [], [], 0
        for m in range(n):
            hit = jnp.where(routing[0, m] == expert, 1, 0) + jnp.where(routing[1, m] == expert, 1, 0)
            hits.append(hit)
            before.append(count)
            count = count + hit
        return hits, before

    def rel(m):
        return (m // 2 + reach - at) % reach

    hits, before = ranks(me)
    theirs, theirs_before = ranks(other)

    def within(taken, member):
        order, count = [], 0
        for m in range(n):
            keep = taken[m] * jnp.where(m % 2 == member, 1, 0)
            order.append((keep, count))
            count = count + keep
        return order

    give = within(theirs, row)
    take = within(hits, 1 - row)
    give_at, slot_at, slot_other, slot_task, slot_valid = [], [], [], [], []
    for slot in range(capacity):
        place = 0
        for m in range(n):
            keep, count = give[m]
            place = place + keep * jnp.where(count == slot, 1, 0) * rel(m)
        give_at.append(jnp.clip(place, 0, reach - 1))
        place, against, task, valid = 0, 0, 0, 0
        for m in range(n):
            here = hits[m] * jnp.where(before[m] == slot, 1, 0)
            near = jnp.where(m % 2 == row, 1, 0)
            place = place + here * (near * rel(m) + (1 - near) * (reach + take[m][1]))
            against = against + here * (routing[0, m] + routing[1, m] - me)
            task = task + here * tasks[m]
            valid = valid + here
        slot_at.append(jnp.clip(place, 0, reach + capacity - 1))
        slot_other.append(against)
        slot_task.append(task)
        slot_valid.append(valid)

    def slot_of(taken, earlier, j, base):
        e = ((at + j) % reach) * 2 + row
        place = 0
        for m in range(n):
            here = taken[m] * jnp.where(m == e, 1, 0)
            place = place + here * (base + earlier[m] - 2 * capacity)
        return jnp.clip(place + 2 * capacity, 0, 2 * capacity)

    mine_for = [slot_of(hits, before, j, 0) for j in range(reach)]
    pair_for = [slot_of(theirs, theirs_before, j, capacity) for j in range(reach)]

    def y_copy(c):
        return remote(picked.at[c], given.at[c], ys.at[c], yr.at[c], pair)

    def x_copy(c, k):
        return remote(
            cols.at[c, 0, 0], cols.at[c, chips - k, 0], x_s.at[c, k], x_r.at[c, chips - k], chip(k)
        )

    def x_recv(c, k):
        return remote(
            cols.at[c, 0, 0], cols.at[c, k, 0], x_s.at[c, chips - k], x_r.at[c, k], chip(chips - k)
        )

    def b_copy(c, k):
        return remote(cols.at[c, k, 0], cols.at[c, k, 1], b_s.at[c, k], b_r.at[c, k], sibling)

    def p_copy(c, k):
        return remote(pout.at[c, k], pin.at[c, k], p_s.at[c, k], p_r.at[c, k], sibling)

    def q_copy(c, k):
        return remote(xs.at[c, k], xr.at[c, chips - k], q_s.at[c, k], q_r.at[c, chips - k], chip(k))

    def q_recv(c, k):
        return remote(xs.at[c, chips - k], xr.at[c, k], q_s.at[c, chips - k], q_r.at[c, k], chip(chips - k))

    def v_copy(c):
        return remote(
            gated[c].at[pl.ds(0, capacity)], gated[c].at[pl.ds(capacity, capacity)], v_s.at[c], v_r.at[c], pair
        )

    def u_copy(c, j):
        return remote(shares.at[c, j], landed.at[c, reach - j], u_s.at[c, j], u_r.at[c, reach - j], peer(j))

    def y_stage(c):
        for j in range(1, reach):
            z_copy(c, reach - j).wait_recv()
        line[c][0] = tokens[span(c), :]
        for slot in range(capacity):
            picked[c, slot] = line[c][give_at[slot]]
        go(y_copy(c))

    def x_stage(c):
        y_copy(c).wait_recv()
        line[c][reach:] = given[c]
        for slot in range(capacity):
            cols[c, 0, 0, slot * ROWS : (slot + 1) * ROWS, :] = line[c][slot_at[slot]]
        for k in range(1, chips):
            go(x_copy(c, k))
        go(b_copy(c, 0))
        if c == 0:
            loads[3].wait()
        logits = lax.dot_general(
            cols[c, 0, 0], gate_weight[...], (((1,), (1,)), ((), ())), preferred_element_type=jnp.float32
        )
        column = lax.broadcasted_iota(jnp.int32, (ROWS, logits.shape[1]), 1)
        for slot in range(capacity):
            own = slot_task[slot] * n + me
            against = slot_task[slot] * n + slot_other[slot]
            sign = jnp.where(column == own, 1.0, 0.0) - jnp.where(column == against, 1.0, 0.0)
            gap = jnp.sum(logits[slot * ROWS : (slot + 1) * ROWS] * sign, axis=1, keepdims=True)
            gate = jax.nn.sigmoid(gap) * slot_valid[slot].astype(jnp.float32)
            weights[c, slot * ROWS : (slot + 1) * ROWS, :] = jnp.broadcast_to(gate, (ROWS, 128))

    def relay_stage(c):
        for k in range(1, chips):
            x_recv(c, k).wait_recv()
            go(b_copy(c, k))

    def expert_stage(c):
        if c == 0:
            loads[1].wait()
            loads[2].wait()
        for k in range(chips):
            b_copy(c, k).wait_recv()
        lhs = cols.at[c]
        tall = chips * 2 * wide

        x = lhs[...].reshape(tall, d_model)
        y = jnp.dot(x, w_in[...], preferred_element_type=jnp.float32)
        hidden[...] = gelu(y).astype(jnp.bfloat16)
        y = jnp.dot(hidden[...], w_out[...], preferred_element_type=jnp.float32)
        for k in range(chips - 1, -1, -1):
            acc[c, k] = y[2 * k * wide : (2 * k + 1) * wide]
            pout[c, k] = y[(2 * k + 1) * wide : (2 * k + 2) * wide].astype(jnp.bfloat16)
            go(p_copy(c, k))

    def back_stage(c):
        for k in range(1, chips):
            p_copy(c, k).wait_recv()
            xs[c, k] = (acc[c, k] + pin[c, k].astype(jnp.float32)).astype(jnp.bfloat16)
            go(q_copy(c, k))

    def gate_stage(c):
        p_copy(c, 0).wait_recv()
        for k in range(1, chips):
            q_recv(c, k).wait_recv()
        for slot in range(capacity):
            rows = slice(slot * ROWS, (slot + 1) * ROWS)
            total = acc[c, 0, rows, :] + pin[c, 0, rows, :].astype(jnp.float32)
            for k in range(1, chips):
                total = total + xr[c, k, rows, :].astype(jnp.float32)
            gated[c][slot] = (weights[c, rows, :1] * total).astype(jnp.bfloat16)
        gated[c][2 * capacity] = jnp.zeros((ROWS, d_model), jnp.bfloat16)
        go(v_copy(c))

    def share(c, j):
        return gated[c][mine_for[j]].astype(jnp.float32) + gated[c][pair_for[j]].astype(jnp.float32)

    def share_stage(c):
        v_copy(c).wait_recv()
        for j in range(1, reach):
            shares[c, j] = share(c, j).astype(jnp.bfloat16)
            go(u_copy(c, j))

    def out_copy(c):
        return pltpu.make_async_copy(result.at[pl.ds(c * ROWS, ROWS)], out_hbm.at[pl.ds(c * ROWS, ROWS)], o_s.at[c])

    def out_stage(c):
        total = share(c, 0)
        for j in range(1, reach):
            u_copy(c, reach - j).wait_recv()
            total = total + landed[c, j].astype(jnp.float32)
        result[span(c), :] = total.astype(jnp.bfloat16)
        out_copy(c).start()

    stages = {
        "y": y_stage, "x": x_stage, "relay": relay_stage, "expert": expert_stage,
        "back": back_stage, "gate": gate_stage, "share": share_stage, "out": out_stage,
    }
    plan = []
    for c in range(parts):
        for name in stages:
            plan.append((LAGS[name] + c, len(plan), name, c))
    for _, _, name, c in sorted(plan):
        stages[name](c)
    for copy in sent:
        copy.wait_send()
    for c in range(parts):
        out_copy(c).wait()


def shards(tokens, task_ids, routing, gate_weight, w_in, w_out):
    n = lax.axis_size("expert")
    n_dp = lax.axis_size("dp")
    d_model = tokens.shape[1]
    capacity = 2 * (tokens.shape[0] // BLK) + 1
    chips, reach = n_dp // 2, n // 2
    parts = BLK // ROWS
    wide = capacity * ROWS
    bf16 = jnp.bfloat16
    dma = pltpu.SemaphoreType.DMA
    hbm = pl.BlockSpec(memory_space=pl.ANY)
    return pl.pallas_call(
        functools.partial(kernel, n, n_dp, capacity),
        out_shape=jax.ShapeDtypeStruct(tokens.shape, bf16),
        in_specs=[hbm] * 6,
        out_specs=hbm,
        scratch_shapes=[
            pltpu.SMEM(routing.shape[::-1], jnp.int32),
            pltpu.SMEM(task_ids.shape, jnp.int32),
            pltpu.VMEM(tokens.shape, bf16),
            pltpu.VMEM(gate_weight.shape[::-1], bf16),
            pltpu.VMEM(w_in.shape[1:], bf16),
            pltpu.VMEM(w_out.shape[1:], bf16),
            [pltpu.VMEM((reach + capacity, ROWS, d_model), bf16) for _ in range(parts)],
            pltpu.VMEM((parts, capacity, ROWS, d_model), bf16),
            pltpu.VMEM((parts, capacity, ROWS, d_model), bf16),
            pltpu.VMEM((parts, chips, 2, wide, d_model), bf16),
            pltpu.VMEM((chips * 2 * wide, w_in.shape[2]), bf16),
            pltpu.VMEM((parts, chips, wide, d_model), jnp.float32),
            pltpu.VMEM((parts, chips, wide, d_model), bf16),
            pltpu.VMEM((parts, chips, wide, d_model), bf16),
            pltpu.VMEM((parts, chips, wide, d_model), bf16),
            pltpu.VMEM((parts, chips, wide, d_model), bf16),
            [pltpu.VMEM((2 * capacity + 1, ROWS, d_model), bf16) for _ in range(parts)],
            pltpu.VMEM((parts, wide, 128), jnp.float32),
            pltpu.VMEM((parts, reach, ROWS, d_model), bf16),
            pltpu.VMEM((parts, reach, ROWS, d_model), bf16),
            pltpu.VMEM(tokens.shape, bf16),
            dma((6,)),
            dma((parts, reach)),
            dma((parts, reach)),
            dma((parts,)),
            dma((parts,)),
            dma((parts, chips)),
            dma((parts, chips)),
            dma((parts, chips)),
            dma((parts, chips)),
            dma((parts, chips)),
            dma((parts, chips)),
            dma((parts, chips)),
            dma((parts, chips)),
            dma((parts,)),
            dma((parts,)),
            dma((parts, reach)),
            dma((parts, reach)),
            dma((parts,)),
        ],
        compiler_params=pltpu.CompilerParams(
            collective_id=0, has_side_effects=True, vmem_limit_bytes=64 * 1024 * 1024 - 65536
        ),
    )(routing.T, task_ids, tokens, gate_weight.T, w_in, w_out)


def solution(mesh):
    placed = (
        P(("dp", "expert"), None),
        P("dp"),
        P("dp", None),
        P(),
        P("expert", None, "dp"),
        P("expert", "dp", None),
    )
    return jax.shard_map(
        shards, mesh=mesh, in_specs=placed, out_specs=P(("dp", "expert"), None), check_vma=False
    )
```

```python
import functools

import jax
import jax.numpy as jnp
from jax import lax
from jax.experimental import pallas as pl
from jax.experimental.pallas import tpu as pltpu
from jax.sharding import PartitionSpec as P

BLK = 128
ROWS = 16
MESH = pl.DeviceIdType.MESH
LAGS = {"y": 0, "x": 1.25, "relay": 2.5, "expert": 2.9, "back": 3.6, "gate": 4.9, "share": 6.2, "out": 20}


def gelu(x):
    return 0.5 * x * (1.0 + jnp.tanh(0.7978845608028654 * (x + 0.044715 * (x * x * x))))


def kernel(
    n, n_dp, capacity,
    routing_hbm, tasks_hbm, tokens_hbm, gate_hbm, w_in_hbm, w_out_hbm, out_hbm,
    routing, tasks, tokens, gate_weight, w_in, w_out, line, picked, given, cols, hidden, acc, pout, pin, xs, xr, gated,
    weights, shares, landed, result,
    ld, zs, zr, ys, yr, x_s, x_r, b_s, b_r, p_s, p_r, q_s, q_r, v_s, v_r, u_s, u_r, o_s,
):
    d_model = tokens.shape[1]
    parts = BLK // ROWS
    chips = n_dp // 2
    reach = n // 2
    wide = capacity * ROWS
    me = lax.axis_index("expert")
    my_dp = lax.axis_index("dp")
    my_x, my_core = my_dp // 2, my_dp % 2
    at, row = me // 2, me % 2
    other = me + 1 - 2 * row
    pair = {"expert": other}
    sibling = {"dp": my_x * 2 + 1 - my_core}

    def peer(j):
        return {"expert": ((at + j) % reach) * 2 + row}

    def chip(k):
        return {"dp": ((my_x + k) % chips) * 2 + my_core}

    loads = [
        pltpu.make_async_copy(tokens_hbm, tokens, ld.at[0]),
        pltpu.make_async_copy(w_in_hbm.at[0], w_in, ld.at[1]),
        pltpu.make_async_copy(w_out_hbm.at[0], w_out, ld.at[2]),
        pltpu.make_async_copy(gate_hbm, gate_weight, ld.at[3]),
        pltpu.make_async_copy(routing_hbm, routing, ld.at[4]),
        pltpu.make_async_copy(tasks_hbm, tasks, ld.at[5]),
    ]
    for load in [loads[0]] + loads[4:] + loads[1:4]:
        load.start()

    barrier = pltpu.get_barrier_semaphore()
    partners = [peer(j) for j in range(1, reach)] + [pair, sibling] + [chip(k) for k in range(1, chips)]
    for partner in partners:
        pl.semaphore_signal(barrier, inc=1, device_id=partner, device_id_type=MESH)
    pl.semaphore_wait(barrier, len(partners))

    def remote(src, dst, send, recv, target):
        return pltpu.make_async_remote_copy(
            src_ref=src, dst_ref=dst, send_sem=send, recv_sem=recv,
            device_id=target, device_id_type=MESH,
        )

    sent = []

    def go(copy):
        copy.start()
        sent.append(copy)

    def span(c):
        return slice(c * ROWS, (c + 1) * ROWS)

    def z_copy(c, j):
        return remote(
            tokens.at[pl.ds(c * ROWS, ROWS)], line[c].at[reach - j], zs.at[c, j], zr.at[c, reach - j], peer(j)
        )

    loads[0].wait()
    for c in range(parts):
        for j in range(1, reach):
            go(z_copy(c, j))

    loads[4].wait()
    loads[5].wait()

    def ranks(expert):
        hits, before, count = [], [], 0
        for m in range(n):
            hit = jnp.where(routing[0, m] == expert, 1, 0) + jnp.where(routing[1, m] == expert, 1, 0)
            hits.append(hit)
            before.append(count)
            count = count + hit
        return hits, before

    def rel(m):
        return (m // 2 + reach - at) % reach

    hits, before = ranks(me)
    theirs, theirs_before = ranks(other)

    def within(taken, member):
        order, count = [], 0
        for m in range(n):
            keep = taken[m] * jnp.where(m % 2 == member, 1, 0)
            order.append((keep, count))
            count = count + keep
        return order

    give = within(theirs, row)
    take = within(hits, 1 - row)
    give_at, slot_at, slot_other, slot_task, slot_valid = [], [], [], [], []
    for slot in range(capacity):
        place = 0
        for m in range(n):
            keep, count = give[m]
            place = place + keep * jnp.where(count == slot, 1, 0) * rel(m)
        give_at.append(jnp.clip(place, 0, reach - 1))
        place, against, task, valid = 0, 0, 0, 0
        for m in range(n):
            here = hits[m] * jnp.where(before[m] == slot, 1, 0)
            near = jnp.where(m % 2 == row, 1, 0)
            place = place + here * (near * rel(m) + (1 - near) * (reach + take[m][1]))
            against = against + here * (routing[0, m] + routing[1, m] - me)
            task = task + here * tasks[m]
            valid = valid + here
        slot_at.append(jnp.clip(place, 0, reach + capacity - 1))
        slot_other.append(against)
        slot_task.append(task)
        slot_valid.append(valid)

    def slot_of(taken, earlier, j, base):
        e = ((at + j) % reach) * 2 + row
        place = 0
        for m in range(n):
            here = taken[m] * jnp.where(m == e, 1, 0)
            place = place + here * (base + earlier[m] - 2 * capacity)
        return jnp.clip(place + 2 * capacity, 0, 2 * capacity)

    mine_for = [slot_of(hits, before, j, 0) for j in range(reach)]
    pair_for = [slot_of(theirs, theirs_before, j, capacity) for j in range(reach)]

    def y_copy(c):
        return remote(picked.at[c], given.at[c], ys.at[c], yr.at[c], pair)

    def x_copy(c, k):
        return remote(
            cols.at[c, 0, 0], cols.at[c, chips - k, 0], x_s.at[c, k], x_r.at[c, chips - k], chip(k)
        )

    def x_recv(c, k):
        return remote(
            cols.at[c, 0, 0], cols.at[c, k, 0], x_s.at[c, chips - k], x_r.at[c, k], chip(chips - k)
        )

    def b_copy(c, k):
        return remote(cols.at[c, k, 0], cols.at[c, k, 1], b_s.at[c, k], b_r.at[c, k], sibling)

    def p_copy(c, k):
        return remote(pout.at[c, k], pin.at[c, k], p_s.at[c, k], p_r.at[c, k], sibling)

    def q_copy(c, k):
        return remote(xs.at[c, k], xr.at[c, chips - k], q_s.at[c, k], q_r.at[c, chips - k], chip(k))

    def q_recv(c, k):
        return remote(xs.at[c, chips - k], xr.at[c, k], q_s.at[c, chips - k], q_r.at[c, k], chip(chips - k))

    def v_copy(c):
        return remote(
            gated[c].at[pl.ds(0, capacity)], gated[c].at[pl.ds(capacity, capacity)], v_s.at[c], v_r.at[c], pair
        )

    def u_copy(c, j):
        return remote(shares.at[c, j], landed.at[c, reach - j], u_s.at[c, j], u_r.at[c, reach - j], peer(j))

    def y_stage(c):
        for j in range(1, reach):
            z_copy(c, reach - j).wait_recv()
        line[c][0] = tokens[span(c), :]
        for slot in range(capacity):
            picked[c, slot] = line[c][give_at[slot]]
        go(y_copy(c))

    def x_stage(c):
        y_copy(c).wait_recv()
        line[c][reach:] = given[c]
        for slot in range(capacity):
            cols[c, 0, 0, slot * ROWS : (slot + 1) * ROWS, :] = line[c][slot_at[slot]]
        for k in range(1, chips):
            go(x_copy(c, k))
        go(b_copy(c, 0))
        if c == 0:
            loads[3].wait()
        logits = lax.dot_general(
            cols[c, 0, 0], gate_weight[...], (((1,), (1,)), ((), ())), preferred_element_type=jnp.float32
        )
        column = lax.broadcasted_iota(jnp.int32, (ROWS, logits.shape[1]), 1)
        for slot in range(capacity):
            own = slot_task[slot] * n + me
            against = slot_task[slot] * n + slot_other[slot]
            sign = jnp.where(column == own, 1.0, 0.0) - jnp.where(column == against, 1.0, 0.0)
            gap = jnp.sum(logits[slot * ROWS : (slot + 1) * ROWS] * sign, axis=1, keepdims=True)
            gate = jax.nn.sigmoid(gap) * slot_valid[slot].astype(jnp.float32)
            weights[c, slot * ROWS : (slot + 1) * ROWS, :] = jnp.broadcast_to(gate, (ROWS, 128))

    def relay_stage(c):
        for k in range(1, chips):
            x_recv(c, k).wait_recv()
            go(b_copy(c, k))

    def expert_stage(c):
        if c == 0:
            loads[1].wait()
            loads[2].wait()
        for k in range(chips):
            b_copy(c, k).wait_recv()
        lhs = cols.at[c]
        tall = chips * 2 * wide

        x = lhs[...].reshape(tall, d_model)
        y = jnp.dot(x, w_in[...], preferred_element_type=jnp.float32)
        hidden[...] = gelu(y).astype(jnp.bfloat16)
        y = jnp.dot(hidden[...], w_out[...], preferred_element_type=jnp.float32)
        for k in range(chips - 1, -1, -1):
            acc[c, k] = y[2 * k * wide : (2 * k + 1) * wide]
            pout[c, k] = y[(2 * k + 1) * wide : (2 * k + 2) * wide].astype(jnp.bfloat16)
            go(p_copy(c, k))

    def back_stage(c):
        for k in range(1, chips):
            p_copy(c, k).wait_recv()
            xs[c, k] = (acc[c, k] + pin[c, k].astype(jnp.float32)).astype(jnp.bfloat16)
            go(q_copy(c, k))

    def gate_stage(c):
        p_copy(c, 0).wait_recv()
        for k in range(1, chips):
            q_recv(c, k).wait_recv()
        for slot in range(capacity):
            rows = slice(slot * ROWS, (slot + 1) * ROWS)
            total = acc[c, 0, rows, :] + pin[c, 0, rows, :].astype(jnp.float32)
            for k in range(1, chips):
                total = total + xr[c, k, rows, :].astype(jnp.float32)
            gated[c][slot] = (weights[c, rows, :1] * total).astype(jnp.bfloat16)
        gated[c][2 * capacity] = jnp.zeros((ROWS, d_model), jnp.bfloat16)
        go(v_copy(c))

    def share(c, j):
        return gated[c][mine_for[j]].astype(jnp.float32) + gated[c][pair_for[j]].astype(jnp.float32)

    def share_stage(c):
        v_copy(c).wait_recv()
        for j in range(1, reach):
            shares[c, j] = share(c, j).astype(jnp.bfloat16)
            go(u_copy(c, j))

    def out_copy(c):
        return pltpu.make_async_copy(result.at[pl.ds(c * ROWS, ROWS)], out_hbm.at[pl.ds(c * ROWS, ROWS)], o_s.at[c])

    def out_stage(c):
        total = share(c, 0)
        for j in range(1, reach):
            u_copy(c, reach - j).wait_recv()
            total = total + landed[c, j].astype(jnp.float32)
        result[span(c), :] = total.astype(jnp.bfloat16)
        out_copy(c).start()

    stages = {
        "y": y_stage, "x": x_stage, "relay": relay_stage, "expert": expert_stage,
        "back": back_stage, "gate": gate_stage, "share": share_stage, "out": out_stage,
    }
    plan = []
    for c in range(parts):
        for name in stages:
            plan.append((LAGS[name] + c, len(plan), name, c))
    for _, _, name, c in sorted(plan):
        stages[name](c)
    for copy in sent:
        copy.wait_send()
    for c in range(parts):
        out_copy(c).wait()


def shards(tokens, task_ids, routing, gate_weight, w_in, w_out):
    n = lax.axis_size("expert")
    n_dp = lax.axis_size("dp")
    d_model = tokens.shape[1]
    capacity = 2 * (tokens.shape[0] // BLK) + 1
    chips, reach = n_dp // 2, n // 2
    parts = BLK // ROWS
    wide = capacity * ROWS
    bf16 = jnp.bfloat16
    dma = pltpu.SemaphoreType.DMA
    hbm = pl.BlockSpec(memory_space=pl.ANY)
    return pl.pallas_call(
        functools.partial(kernel, n, n_dp, capacity),
        out_shape=jax.ShapeDtypeStruct(tokens.shape, bf16),
        in_specs=[hbm] * 6,
        out_specs=hbm,
        scratch_shapes=[
            pltpu.SMEM(routing.shape[::-1], jnp.int32),
            pltpu.SMEM(task_ids.shape, jnp.int32),
            pltpu.VMEM(tokens.shape, bf16),
            pltpu.VMEM(gate_weight.shape[::-1], bf16),
            pltpu.VMEM(w_in.shape[1:], bf16),
            pltpu.VMEM(w_out.shape[1:], bf16),
            [pltpu.VMEM((reach + capacity, ROWS, d_model), bf16) for _ in range(parts)],
            pltpu.VMEM((parts, capacity, ROWS, d_model), bf16),
            pltpu.VMEM((parts, capacity, ROWS, d_model), bf16),
            pltpu.VMEM((parts, chips, 2, wide, d_model), bf16),
            pltpu.VMEM((chips * 2 * wide, w_in.shape[2]), bf16),
            pltpu.VMEM((parts, chips, wide, d_model), jnp.float32),
            pltpu.VMEM((parts, chips, wide, d_model), bf16),
            pltpu.VMEM((parts, chips, wide, d_model), bf16),
            pltpu.VMEM((parts, chips, wide, d_model), bf16),
            pltpu.VMEM((parts, chips, wide, d_model), bf16),
            [pltpu.VMEM((2 * capacity + 1, ROWS, d_model), bf16) for _ in range(parts)],
            pltpu.VMEM((parts, wide, 128), jnp.float32),
            pltpu.VMEM((parts, reach, ROWS, d_model), bf16),
            pltpu.VMEM((parts, reach, ROWS, d_model), bf16),
            pltpu.VMEM(tokens.shape, bf16),
            dma((6,)),
            dma((parts, reach)),
            dma((parts, reach)),
            dma((parts,)),
            dma((parts,)),
            dma((parts, chips)),
            dma((parts, chips)),
            dma((parts, chips)),
            dma((parts, chips)),
            dma((parts, chips)),
            dma((parts, chips)),
            dma((parts, chips)),
            dma((parts, chips)),
            dma((parts,)),
            dma((parts,)),
            dma((parts, reach)),
            dma((parts, reach)),
            dma((parts,)),
        ],
        compiler_params=pltpu.CompilerParams(
            collective_id=0, has_side_effects=True, vmem_limit_bytes=64 * 1024 * 1024 - 65536
        ),
    )(routing.T, task_ids, tokens, gate_weight.T, w_in, w_out)


def solution(mesh):
    placed = (
        P(("dp", "expert"), None),
        P("dp"),
        P("dp", None),
        P(),
        P("expert", None, "dp"),
        P("expert", "dp", None),
    )
    return jax.shard_map(
        shards, mesh=mesh, in_specs=placed, out_specs=P(("dp", "expert"), None), check_vma=False
    )
```

```python
import functools

import jax
import jax.numpy as jnp
from jax import lax
from jax.experimental import pallas as pl
from jax.experimental.pallas import tpu as pltpu
from jax.sharding import PartitionSpec as P

BLK = 128
ROWS = 16
STEPS = {"gate": 1.12, "share": 1.12}
MESH = pl.DeviceIdType.MESH
LAGS = {"y": 0, "x": 1.25, "relay": 2.5, "expert": 2.9, "back": 3.6, "gate": 4.9, "share": 6.2, "out": 20}


def gelu(x):
    return 0.5 * x * (1.0 + jnp.tanh(0.7978845608028654 * (x + 0.044715 * (x * x * x))))


def kernel(
    n, n_dp, capacity,
    routing_hbm, tasks_hbm, tokens_hbm, gate_hbm, w_in_hbm, w_out_hbm, out_hbm,
    routing, tasks, tokens, gate_weight, w_in, w_out, line, picked, given, cols, hidden, acc, pout, pin, xs, xr, gated,
    weights, shares, landed, result,
    ld, zs, zr, ys, yr, x_s, x_r, b_s, b_r, p_s, p_r, q_s, q_r, v_s, v_r, u_s, u_r, o_s,
):
    d_model = tokens.shape[1]
    parts = BLK // ROWS
    chips = n_dp // 2
    reach = n // 2
    wide = capacity * ROWS
    me = lax.axis_index("expert")
    my_dp = lax.axis_index("dp")
    my_x, my_core = my_dp // 2, my_dp % 2
    at, row = me // 2, me % 2
    other = me + 1 - 2 * row
    pair = {"expert": other}
    sibling = {"dp": my_x * 2 + 1 - my_core}

    def peer(j):
        return {"expert": ((at + j) % reach) * 2 + row}

    def chip(k):
        return {"dp": ((my_x + k) % chips) * 2 + my_core}

    loads = [
        pltpu.make_async_copy(tokens_hbm, tokens, ld.at[0]),
        pltpu.make_async_copy(w_in_hbm.at[0], w_in, ld.at[1]),
        pltpu.make_async_copy(w_out_hbm.at[0], w_out, ld.at[2]),
        pltpu.make_async_copy(gate_hbm, gate_weight, ld.at[3]),
        pltpu.make_async_copy(routing_hbm, routing, ld.at[4]),
        pltpu.make_async_copy(tasks_hbm, tasks, ld.at[5]),
    ]
    for load in [loads[0]] + loads[4:] + loads[1:4]:
        load.start()

    barrier = pltpu.get_barrier_semaphore()
    partners = [peer(j) for j in range(1, reach)] + [pair, sibling] + [chip(k) for k in range(1, chips)]
    for partner in partners:
        pl.semaphore_signal(barrier, inc=1, device_id=partner, device_id_type=MESH)
    pl.semaphore_wait(barrier, len(partners))

    def remote(src, dst, send, recv, target):
        return pltpu.make_async_remote_copy(
            src_ref=src, dst_ref=dst, send_sem=send, recv_sem=recv,
            device_id=target, device_id_type=MESH,
        )

    sent = []

    def go(copy):
        copy.start()
        sent.append(copy)

    def span(c):
        return slice(c * ROWS, (c + 1) * ROWS)

    def z_copy(c, j):
        return remote(
            tokens.at[pl.ds(c * ROWS, ROWS)], line[c].at[reach - j], zs.at[c, j], zr.at[c, reach - j], peer(j)
        )

    loads[0].wait()
    for c in range(parts):
        for j in range(1, reach):
            go(z_copy(c, j))

    loads[4].wait()
    loads[5].wait()

    def ranks(expert):
        hits, before, count = [], [], 0
        for m in range(n):
            hit = jnp.where(routing[0, m] == expert, 1, 0) + jnp.where(routing[1, m] == expert, 1, 0)
            hits.append(hit)
            before.append(count)
            count = count + hit
        return hits, before

    def rel(m):
        return (m // 2 + reach - at) % reach

    hits, before = ranks(me)
    theirs, theirs_before = ranks(other)

    def within(taken, member):
        order, count = [], 0
        for m in range(n):
            keep = taken[m] * jnp.where(m % 2 == member, 1, 0)
            order.append((keep, count))
            count = count + keep
        return order

    give = within(theirs, row)
    take = within(hits, 1 - row)
    give_at, slot_at, slot_other, slot_task, slot_valid = [], [], [], [], []
    for slot in range(capacity):
        place = 0
        for m in range(n):
            keep, count = give[m]
            place = place + keep * jnp.where(count == slot, 1, 0) * rel(m)
        give_at.append(jnp.clip(place, 0, reach - 1))
        place, against, task, valid = 0, 0, 0, 0
        for m in range(n):
            here = hits[m] * jnp.where(before[m] == slot, 1, 0)
            near = jnp.where(m % 2 == row, 1, 0)
            place = place + here * (near * rel(m) + (1 - near) * (reach + take[m][1]))
            against = against + here * (routing[0, m] + routing[1, m] - me)
            task = task + here * tasks[m]
            valid = valid + here
        slot_at.append(jnp.clip(place, 0, reach + capacity - 1))
        slot_other.append(against)
        slot_task.append(task)
        slot_valid.append(valid)

    def slot_of(taken, earlier, j, base):
        e = ((at + j) % reach) * 2 + row
        place = 0
        for m in range(n):
            here = taken[m] * jnp.where(m == e, 1, 0)
            place = place + here * (base + earlier[m] - 2 * capacity)
        return jnp.clip(place + 2 * capacity, 0, 2 * capacity)

    mine_for = [slot_of(hits, before, j, 0) for j in range(reach)]
    pair_for = [slot_of(theirs, theirs_before, j, capacity) for j in range(reach)]

    def y_copy(c):
        return remote(picked.at[c], given.at[c], ys.at[c], yr.at[c], pair)

    def x_copy(c, k):
        return remote(
            cols.at[c, 0, 0], cols.at[c, chips - k, 0], x_s.at[c, k], x_r.at[c, chips - k], chip(k)
        )

    def x_recv(c, k):
        return remote(
            cols.at[c, 0, 0], cols.at[c, k, 0], x_s.at[c, chips - k], x_r.at[c, k], chip(chips - k)
        )

    def b_copy(c, k):
        return remote(cols.at[c, k, 0], cols.at[c, k, 1], b_s.at[c, k], b_r.at[c, k], sibling)

    def p_copy(c, k):
        return remote(pout.at[c, k], pin.at[c, k], p_s.at[c, k], p_r.at[c, k], sibling)

    def q_copy(c, k):
        return remote(xs.at[c, k], xr.at[c, chips - k], q_s.at[c, k], q_r.at[c, chips - k], chip(k))

    def q_recv(c, k):
        return remote(xs.at[c, chips - k], xr.at[c, k], q_s.at[c, chips - k], q_r.at[c, k], chip(chips - k))

    def v_copy(c):
        return remote(
            gated[c].at[pl.ds(0, capacity)], gated[c].at[pl.ds(capacity, capacity)], v_s.at[c], v_r.at[c], pair
        )

    def u_copy(c, j):
        return remote(shares.at[c, j], landed.at[c, reach - j], u_s.at[c, j], u_r.at[c, reach - j], peer(j))

    def y_stage(c):
        for j in range(1, reach):
            z_copy(c, reach - j).wait_recv()
        line[c][0] = tokens[span(c), :]
        for slot in range(capacity):
            picked[c, slot] = line[c][give_at[slot]]
        go(y_copy(c))

    def x_stage(c):
        y_copy(c).wait_recv()
        line[c][reach:] = given[c]
        for slot in range(capacity):
            cols[c, 0, 0, slot * ROWS : (slot + 1) * ROWS, :] = line[c][slot_at[slot]]
        for k in range(1, chips):
            go(x_copy(c, k))
        go(b_copy(c, 0))
        if c == 0:
            loads[3].wait()
        logits = lax.dot_general(
            cols[c, 0, 0], gate_weight[...], (((1,), (1,)), ((), ())), preferred_element_type=jnp.float32
        )
        column = lax.broadcasted_iota(jnp.int32, (ROWS, logits.shape[1]), 1)
        for slot in range(capacity):
            own = slot_task[slot] * n + me
            against = slot_task[slot] * n + slot_other[slot]
            sign = jnp.where(column == own, 1.0, 0.0) - jnp.where(column == against, 1.0, 0.0)
            gap = jnp.sum(logits[slot * ROWS : (slot + 1) * ROWS] * sign, axis=1, keepdims=True)
            gate = jax.nn.sigmoid(gap) * slot_valid[slot].astype(jnp.float32)
            weights[c, slot * ROWS : (slot + 1) * ROWS, :] = jnp.broadcast_to(gate, (ROWS, 128))

    def relay_stage(c):
        for k in range(1, chips):
            x_recv(c, k).wait_recv()
            go(b_copy(c, k))

    def expert_stage(c):
        if c == 0:
            loads[1].wait()
            loads[2].wait()
        for k in range(chips):
            b_copy(c, k).wait_recv()
        lhs = cols.at[c]
        tall = chips * 2 * wide

        x = lhs[...].reshape(tall, d_model)
        y = jnp.dot(x, w_in[...], preferred_element_type=jnp.float32)
        hidden[...] = gelu(y).astype(jnp.bfloat16)
        y = jnp.dot(hidden[...], w_out[...], preferred_element_type=jnp.float32)
        for k in range(chips - 1, -1, -1):
            acc[c, k] = y[2 * k * wide : (2 * k + 1) * wide]
            pout[c, k] = y[(2 * k + 1) * wide : (2 * k + 2) * wide].astype(jnp.bfloat16)
            go(p_copy(c, k))

    def back_stage(c):
        for k in range(1, chips):
            p_copy(c, k).wait_recv()
            xs[c, k] = (acc[c, k] + pin[c, k].astype(jnp.float32)).astype(jnp.bfloat16)
            go(q_copy(c, k))

    def gate_stage(c):
        p_copy(c, 0).wait_recv()
        for k in range(1, chips):
            q_recv(c, k).wait_recv()
        for slot in range(capacity):
            rows = slice(slot * ROWS, (slot + 1) * ROWS)
            total = acc[c, 0, rows, :] + pin[c, 0, rows, :].astype(jnp.float32)
            for k in range(1, chips):
                total = total + xr[c, k, rows, :].astype(jnp.float32)
            gated[c][slot] = (weights[c, rows, :1] * total).astype(jnp.bfloat16)
        gated[c][2 * capacity] = jnp.zeros((ROWS, d_model), jnp.bfloat16)
        go(v_copy(c))

    def share(c, j):
        return gated[c][mine_for[j]].astype(jnp.float32) + gated[c][pair_for[j]].astype(jnp.float32)

    def share_stage(c):
        v_copy(c).wait_recv()
        for j in range(1, reach):
            shares[c, j] = share(c, j).astype(jnp.bfloat16)
            go(u_copy(c, j))

    def out_copy(c):
        return pltpu.make_async_copy(result.at[pl.ds(c * ROWS, ROWS)], out_hbm.at[pl.ds(c * ROWS, ROWS)], o_s.at[c])

    def out_stage(c):
        total = share(c, 0)
        for j in range(1, reach):
            u_copy(c, reach - j).wait_recv()
            total = total + landed[c, j].astype(jnp.float32)
        result[span(c), :] = total.astype(jnp.bfloat16)
        out_copy(c).start()

    stages = {
        "y": y_stage, "x": x_stage, "relay": relay_stage, "expert": expert_stage,
        "back": back_stage, "gate": gate_stage, "share": share_stage, "out": out_stage,
    }
    plan = []
    for c in range(parts):
        for name in stages:
            plan.append((LAGS[name] + STEPS.get(name, 1.0) * c, len(plan), name, c))
    for _, _, name, c in sorted(plan):
        stages[name](c)
    for copy in sent:
        copy.wait_send()
    for c in range(parts):
        out_copy(c).wait()


def shards(tokens, task_ids, routing, gate_weight, w_in, w_out):
    n = lax.axis_size("expert")
    n_dp = lax.axis_size("dp")
    d_model = tokens.shape[1]
    capacity = 2 * (tokens.shape[0] // BLK) + 1
    chips, reach = n_dp // 2, n // 2
    parts = BLK // ROWS
    wide = capacity * ROWS
    bf16 = jnp.bfloat16
    dma = pltpu.SemaphoreType.DMA
    hbm = pl.BlockSpec(memory_space=pl.ANY)
    return pl.pallas_call(
        functools.partial(kernel, n, n_dp, capacity),
        out_shape=jax.ShapeDtypeStruct(tokens.shape, bf16),
        in_specs=[hbm] * 6,
        out_specs=hbm,
        scratch_shapes=[
            pltpu.SMEM(routing.shape[::-1], jnp.int32),
            pltpu.SMEM(task_ids.shape, jnp.int32),
            pltpu.VMEM(tokens.shape, bf16),
            pltpu.VMEM(gate_weight.shape[::-1], bf16),
            pltpu.VMEM(w_in.shape[1:], bf16),
            pltpu.VMEM(w_out.shape[1:], bf16),
            [pltpu.VMEM((reach + capacity, ROWS, d_model), bf16) for _ in range(parts)],
            pltpu.VMEM((parts, capacity, ROWS, d_model), bf16),
            pltpu.VMEM((parts, capacity, ROWS, d_model), bf16),
            pltpu.VMEM((parts, chips, 2, wide, d_model), bf16),
            pltpu.VMEM((chips * 2 * wide, w_in.shape[2]), bf16),
            pltpu.VMEM((parts, chips, wide, d_model), jnp.float32),
            pltpu.VMEM((parts, chips, wide, d_model), bf16),
            pltpu.VMEM((parts, chips, wide, d_model), bf16),
            pltpu.VMEM((parts, chips, wide, d_model), bf16),
            pltpu.VMEM((parts, chips, wide, d_model), bf16),
            [pltpu.VMEM((2 * capacity + 1, ROWS, d_model), bf16) for _ in range(parts)],
            pltpu.VMEM((parts, wide, 128), jnp.float32),
            pltpu.VMEM((parts, reach, ROWS, d_model), bf16),
            pltpu.VMEM((parts, reach, ROWS, d_model), bf16),
            pltpu.VMEM(tokens.shape, bf16),
            dma((6,)),
            dma((parts, reach)),
            dma((parts, reach)),
            dma((parts,)),
            dma((parts,)),
            dma((parts, chips)),
            dma((parts, chips)),
            dma((parts, chips)),
            dma((parts, chips)),
            dma((parts, chips)),
            dma((parts, chips)),
            dma((parts, chips)),
            dma((parts, chips)),
            dma((parts,)),
            dma((parts,)),
            dma((parts, reach)),
            dma((parts, reach)),
            dma((parts,)),
        ],
        compiler_params=pltpu.CompilerParams(
            collective_id=0, has_side_effects=True, vmem_limit_bytes=64 * 1024 * 1024 - 65536
        ),
    )(routing.T, task_ids, tokens, gate_weight.T, w_in, w_out)


def solution(mesh):
    placed = (
        P(("dp", "expert"), None),
        P("dp"),
        P("dp", None),
        P(),
        P("expert", None, "dp"),
        P("expert", "dp", None),
    )
    return jax.shard_map(
        shards, mesh=mesh, in_specs=placed, out_specs=P(("dp", "expert"), None), check_vma=False
    )
```
